256 devices in a mesh: owner: 16 (over y, x), rows: 16 (over z, core).
Axes of the slice: x: 4, y: 4, z: 8, core: 2. Of those that a mesh axis runs over, the one named last changes fastest.
Arguments:
- train_gate: float32 [64, 2048, 1024], P('owner', 'rows'), may hold values from -0.1875 to 0.1875
- train_up: float32 [64, 2048, 1024], P('owner', 'rows'), may hold values from -0.1875 to 0.1875
- train_down: float32 [64, 1024, 2048], P('owner', None, 'rows'), may hold values from -0.25 to 0.25
- router_weight: float32 [2048, 64], P('rows', 'owner'), may hold values from -0.125 to 0.125
- router_gain: float32 [2048], P('rows'), may hold values from 0.25 to 1.75
Outputs:
- ready_gate: bfloat16 [64, 2048, 1024], P('owner', None, 'rows')
- ready_up: bfloat16 [64, 2048, 1024], P('owner', None, 'rows')
- ready_down: bfloat16 [64, 1024, 2048], P('owner', 'rows')
- scale_gate: float32 [64, 1024], P('owner', 'rows')
- scale_up: float32 [64, 1024], P('owner', 'rows')
- scale_down: float32 [64, 1024], P('owner', 'rows')
- serve_router: bfloat16 [2048, 64], replicated
The draws below stay inside these ranges and needn't reach their ends.
All inputs are finite; a program needn't handle non-finite values. Where the reference program divides by a largest or mean magnitude, that divisor is 1e-20 or more.
Results may differ from the reference program's by a relative error of at most 0.0013.
Values may be sent and summed in bfloat16 or wider, within the bound.
A program may use at most 64 MiB of HBM per device.

```python
import jax
import jax.numpy as jnp

EXPERTS = 64
D_MODEL = 2048
D_EXPERT = 1024


def raised(drawn, own_key, source, target, parts, factor):
    owner, partner = [(jnp.arange(drawn.shape[axis_at]) // (drawn.shape[axis_at] // parts)).reshape([-1 if axis == axis_at else 1 for axis in range(drawn.ndim)]) for axis_at in (source, target)]
    chosen = jax.random.permutation(own_key, parts)[partner]
    strong = (owner == chosen) | (owner == (partner + parts // 2) % parts)
    return jnp.where(strong, factor * drawn, drawn)


def steps_of(rng, dims, shards, low, top_value):
    def one(dim, parts):
        heights = jax.random.uniform(jax.random.fold_in(jax.random.fold_in(rng, 6), dim), (parts,), jnp.float32, low / len(shards), top_value / len(shards))
        return jnp.repeat(jnp.exp(heights), dims[dim] // parts).reshape((-1,) + (1,) * (len(dims) - dim - 1))

    factor_of = one(*shards[0])
    for cut in shards[1:]:
        factor_of = factor_of * one(*cut)
    return factor_of


def bell_draw(own_key, shape, scale, reach, pieces=(), dtype=jnp.bfloat16):
    result = scale * jax.random.normal(own_key, shape, jnp.float32)
    if pieces:
        result = result * steps_of(own_key, shape, pieces, -0.22, 0.18)
    return jnp.clip(result, -reach, reach).astype(dtype)


def bell_draw_with(own_key, dims, deviation, reach, split, heavy, kind=jnp.bfloat16):
    result = deviation * jax.random.normal(own_key, dims, jnp.float32)
    if split:
        result = result * steps_of(own_key, dims, split, -0.22, 0.18)
    return jnp.clip(raised(result, jax.random.fold_in(own_key, 3), *heavy), -reach, reach).astype(kind)


def setup_inputs(seed: int = 0) -> dict:
    splits = jax.random.split(jax.random.key(seed), 6)
    train_gate = bell_draw_with(splits[0], (EXPERTS, D_MODEL, D_EXPERT), D_MODEL ** -0.5, 0.1875, ((0, 16), (1, 16)), (1, 2, 16, 2.0), jnp.float32)
    train_up = bell_draw_with(splits[1], (EXPERTS, D_MODEL, D_EXPERT), D_MODEL ** -0.5, 0.1875, ((0, 16), (1, 16)), (1, 2, 16, 2.0), jnp.float32)
    train_down = bell_draw_with(splits[2], (EXPERTS, D_EXPERT, D_MODEL), D_EXPERT ** -0.5, 0.25, ((0, 16), (2, 16)), (2, 1, 16, 2.0), jnp.float32)
    router_weight = bell_draw(splits[3], (D_MODEL, EXPERTS), D_MODEL ** -0.5, 0.125, ((0, 16), (1, 16)), jnp.float32)
    router_gain = jnp.clip(1.0 + 0.15 * jax.random.normal(splits[4], (D_MODEL,), jnp.float32), 0.25, 1.75)
    return {"train_gate": train_gate, "train_up": train_up, "train_down": train_down, "router_weight": router_weight, "router_gain": router_gain}


def reference(train_gate, train_up, train_down, router_weight, router_gain):
    scale_gate = jnp.sum(jnp.abs(train_gate), axis=1) / D_MODEL
    ready_gate = (train_gate / jnp.expand_dims(scale_gate, 1)).astype(jnp.bfloat16)
    scale_up = jnp.sum(jnp.abs(train_up), axis=1) / D_MODEL
    ready_up = (train_up / jnp.expand_dims(scale_up, 1)).astype(jnp.bfloat16)
    scale_down = jnp.sum(jnp.abs(train_down), axis=2) / D_MODEL
    ready_down = (train_down / jnp.expand_dims(scale_down, 2)).astype(jnp.bfloat16)
    serve_router = (router_weight * router_gain[:, None]).astype(jnp.bfloat16)
    return ready_gate, ready_up, ready_down, scale_gate, scale_up, scale_down, serve_router
```

```python
import functools

import jax
import jax.numpy as jnp
from jax import lax
from jax.experimental import pallas as pl
from jax.experimental.pallas import tpu as pltpu
from jax.sharding import PartitionSpec as P

D_MODEL = 2048
MESH = pl.DeviceIdType.MESH
F32, BF16 = jnp.float32, jnp.bfloat16

FAR = (4, 3, -3, 2, -2, 1, -1, 0)
PEERS = tuple((dz, dc) for dz in FAR for dc in (0, 1) if (dz, dc) != (0, 0))


def exchange(
    gate, up, down, weight, gain,
    out, scale_gate, scale_up, scale_down, router,
    wide, tall, sent, part0, all0, sums, pieces, total, totals, inverse,
    weight_v, gain_v, mine, column, square,
    load, first_s, first_r, sum_s, sum_r, tot_s, tot_r, main_s, main_r, rt_s, rt_r,
):
    owner, me = lax.axis_index("owner"), lax.axis_index("rows")
    z, c = me // 2, lax.rem(me, 2)
    y, x = owner // 4, lax.rem(owner, 4)

    def peer(dz, dc):
        at = lax.rem(z + dz + 8, 8)
        return at * 2 + (1 - c if dc else c)

    loads = []
    for a in range(12):
        source = (gate, up, down)[a // 4].at[a % 4]
        target = wide.at[a] if a < 8 else tall.at[a - 8]
        loads.append(pltpu.make_async_copy(source, target, load.at[a]))
    small = [
        pltpu.make_async_copy(weight, weight_v, load.at[12]),
        pltpu.make_async_copy(gain, gain_v, load.at[13]),
    ]
    loads[0].start()

    barrier = pltpu.get_barrier_semaphore()
    for dz, dc in PEERS:
        pl.semaphore_signal(barrier, inc=1, device_id={"rows": peer(dz, dc)}, device_id_type=MESH)
    xs = [y * 4 + lax.rem(x + k, 4) for k in (2, 1, 3)]
    ys = [lax.rem(y + k, 4) * 4 + x for k in (2, 1, 3)]
    for o in xs + ys:
        pl.semaphore_signal(barrier, inc=1, device_id={"owner": o}, device_id_type=MESH)
    for copy in loads[1:] + small:
        copy.start()

    eye = lax.broadcasted_iota(jnp.int32, (128, 128), 0) == lax.broadcasted_iota(jnp.int32, (128, 128), 1)

    def wide_sum(a):
        return jnp.sum(jnp.abs(wide[a]), axis=0, keepdims=True)

    loads[0].wait()
    row = wide_sum(0)
    for b in range(8):
        part0[b : b + 1, :] = row[:, b * 128 : (b + 1) * 128]
        pieces[b * 2, 0:1, :] = row[:, b * 128 : (b + 1) * 128]
    pl.semaphore_wait(barrier, len(PEERS) + 6)

    def send(source, target, s, r, to):
        pltpu.make_async_remote_copy(
            src_ref=source, dst_ref=target, send_sem=s, recv_sem=r, device_id=to, device_id_type=MESH
        ).start()

    def finish(ref, sem):
        pltpu.make_async_copy(ref, ref, sem).wait()

    for dz, dc in PEERS:
        send(part0, all0.at[me], first_s, first_r, {"rows": peer(dz, dc)})
    all0[me] = part0[...]

    for a in range(1, 12):
        loads[a].wait()
        if a < 8:
            row = wide_sum(a)
        for b in range(8):
            if a < 8:
                piece = row[:, b * 128 : (b + 1) * 128]
            else:
                column_sum = jnp.sum(jnp.abs(tall[a - 8, b * 128 : (b + 1) * 128, :]), axis=1, keepdims=True)
                piece = jnp.sum(jnp.where(eye, column_sum, 0.0), axis=0, keepdims=True)
            pieces[b * 2 + a // 6, a % 6 : a % 6 + 1, :] = piece
    for dz, dc in PEERS:
        to = peer(dz, dc)
        send(pieces.at[to], sums.at[me], sum_s, sum_r, {"rows": to})
    sums[me] = pieces[me]

    for copy in small:
        copy.wait()
    mine[...] = (weight_v[...] * gain_v[...]).astype(BF16)
    column[me] = mine[...]
    for dz, dc in PEERS:
        send(mine, column.at[me], rt_s.at[0], rt_r.at[0], {"rows": peer(dz, dc)})

    finish(all0.at[pl.ds(0, 15)], first_r)
    first = 1.0 / (jnp.sum(all0[...], axis=0) * (1.0 / D_MODEL))
    for b in range(8):
        inverse[0, b] = first[b : b + 1, :]

    def chunk(a):
        is_wide = not isinstance(a, tuple)
        a = a if is_wide else a[0]
        pending = None
        for dz in FAR:
            at = lax.rem(z + dz + 8, 8)
            rows = pl.ds(pl.multiple_of(at * 128, 128), 128)
            scale = inverse[a, at]
            if is_wide:
                block = (wide[a, :, rows] * scale).astype(BF16).T
            else:
                per_row = jnp.sum(jnp.where(eye, scale, 0.0), axis=1, keepdims=True)
                block = (tall[a - 8, rows, :] * per_row).astype(BF16)
            sent[a, rows, :] = block
            if pending is not None:
                launch(a, pending)
            pending = dz
        launch(a, pending)
        own = sent[a, pl.ds(pl.multiple_of(me * 64, 64), 64), :]
        out[a, :, pl.ds(pl.multiple_of(me * 128, 128), 128)] = own

    def launch(a, dz):
        for dc in (0, 1):
            if (dz, dc) == (0, 0):
                continue
            to = peer(dz, dc)
            send(
                sent.at[a, pl.ds(pl.multiple_of(to * 64, 64), 64), :],
                out.at[a, :, pl.ds(pl.multiple_of(me * 128, 128), 128)],
                main_s.at[a // 4], main_r.at[a // 4], {"rows": to},
            )

    def reduce_sums():
        finish(sums.at[pl.ds(0, 15)], sum_r)
        total[...] = jnp.sum(sums[...], axis=0)
        totals[me] = total[...]
        for dz, dc in PEERS:
            send(total, totals.at[me], tot_s, tot_r, {"rows": peer(dz, dc)})

    reduce_sums()
    chunk(0)

    finish(column.at[pl.ds(0, 15)], rt_r.at[0])
    for r in range(16):
        square[y, x, :, r * 128 : (r + 1) * 128] = column[r]

    finish(totals.at[pl.ds(0, 15)], tot_r)
    for a in range(12):
        for b in range(8):
            if a:
                inverse[a, b] = 1.0 / (totals[b * 2 + a // 6, a % 6 : a % 6 + 1, :] * (1.0 / D_MODEL))

    for o in xs:
        send(square.at[y, x], square.at[y, x], rt_s.at[1], rt_r.at[1], {"owner": o})

    @pl.loop(1, 8)
    def _(a):
        chunk(a)

    finish(square.at[0, pl.ds(0, 3)], rt_r.at[1])
    finish(square.at[0, pl.ds(0, 3)], rt_s.at[1])
    for o in ys:
        send(square.at[y], square.at[y], rt_s.at[2], rt_r.at[2], {"owner": o})

    @pl.loop(8, 12)
    def _(a):
        chunk((a,))

    halves = []
    for h in range(2):
        v = totals[z * 2 + h] * (1.0 / D_MODEL)
        halves.append(jnp.where(c == 1, pltpu.roll(v, 64, 1), v)[:, :64])
    scale_gate[...] = halves[0][:4]
    scale_up[...] = jnp.concatenate([halves[0][4:], halves[1][:2]], axis=0)
    scale_down[...] = halves[1][2:]

    finish(square.at[pl.ds(0, 3)], rt_r.at[2])
    for j in range(4):
        rows16 = jnp.concatenate([square[j, i].astype(F32) for i in range(4)], axis=0)
        router[j * 16 : (j + 1) * 16, :] = rows16.astype(BF16)

    finish(all0.at[pl.ds(0, 15)], first_s)
    finish(sums.at[pl.ds(0, 15)], sum_s)
    finish(totals.at[pl.ds(0, 15)], tot_s)
    finish(column.at[pl.ds(0, 15)], rt_s.at[0])
    finish(square.at[pl.ds(0, 3)], rt_s.at[2])
    for i in range(3):
        finish(out.at[pl.ds(i * 4, 4), :, pl.ds(0, 1920)], main_s.at[i])
        finish(out.at[pl.ds(i * 4, 4), :, pl.ds(0, 1920)], main_r.at[i])


def place(out, scale_gate, scale_up, scale_down, router, *rest):
    outs, sem = rest[:7], rest[7]
    sources = [out.at[pl.ds(0, 4)], out.at[pl.ds(4, 4)], out.at[pl.ds(8, 4)], scale_gate, scale_up, scale_down, router]
    copies = [pltpu.make_async_copy(s, d, sem.at[i]) for i, (s, d) in enumerate(zip(sources, outs))]
    for copy in copies:
        copy.start()
    for copy in copies:
        copy.wait()


def local(train_gate, train_up, train_down, router_weight, router_gain):
    anywhere = pl.BlockSpec(memory_space=pl.ANY)
    vmem = pl.BlockSpec(memory_space=pltpu.VMEM)
    shapes = [((12, 64, 2048), BF16), ((4, 64), F32), ((4, 64), F32), ((4, 64), F32), ((64, 2048), BF16)]
    dma = pltpu.SemaphoreType.DMA
    kept = pl.pallas_call(
        exchange,
        out_shape=[pltpu.VMEM(s, d) for s, d in shapes],
        in_specs=[pl.BlockSpec(memory_space=pltpu.HBM)] * 5,
        out_specs=[vmem] * 5,
        scratch_shapes=[
            pltpu.VMEM((8, 128, 1024), F32),
            pltpu.VMEM((4, 1024, 128), F32),
            pltpu.VMEM((12, 1024, 128), BF16),
            pltpu.VMEM((8, 128), F32),
            pltpu.VMEM((16, 8, 128), F32),
            pltpu.VMEM((16, 6, 128), F32),
            pltpu.VMEM((16, 6, 128), F32),
            pltpu.VMEM((6, 128), F32),
            pltpu.VMEM((16, 6, 128), F32),
            pltpu.VMEM((12, 8, 1, 128), F32),
            pltpu.VMEM((4, 128), F32),
            pltpu.VMEM((1, 128), F32),
            pltpu.VMEM((4, 128), BF16),
            pltpu.VMEM((16, 4, 128), BF16),
            pltpu.VMEM((4, 4, 4, 2048), BF16),
            dma((14,)), dma, dma, dma, dma, dma, dma, dma((3,)), dma((3,)), dma((3,)), dma((3,)),
        ],
        compiler_params=pltpu.CompilerParams(
            collective_id=0, has_side_effects=True, vmem_limit_bytes=58 << 20
        ),
    )(train_gate, train_up, train_down, router_weight.T, router_gain[None])
    outs = [((4, 64, 2048), BF16)] * 3 + [((4, 64), F32)] * 3 + [((64, 2048), BF16)]
    gate, up, down, scale_gate, scale_up, scale_down, router = pl.pallas_call(
        place,
        out_shape=[jax.ShapeDtypeStruct(s, d) for s, d in outs],
        in_specs=[vmem] * 5,
        out_specs=[pl.BlockSpec(memory_space=pltpu.HBM)] * 7,
        scratch_shapes=[dma((7,))],
        compiler_params=pltpu.CompilerParams(vmem_limit_bytes=4 << 20),
    )(*[pltpu.with_memory_space_constraint(k, pltpu.VMEM) for k in kept])
    return (
        jnp.swapaxes(gate, 1, 2), jnp.swapaxes(up, 1, 2), down, scale_gate, scale_up, scale_down, router.T,
    )


def solution(mesh):
    return jax.shard_map(
        local,
        mesh=mesh,
        in_specs=(
            P("owner", "rows", None),
            P("owner", "rows", None),
            P("owner", None, "rows"),
            P("rows", "owner"),
            P("rows"),
        ),
        out_specs=(
            P("owner", None, "rows"),
            P("owner", None, "rows"),
            P("owner", "rows", None),
            P("owner", "rows"),
            P("owner", "rows"),
            P("owner", "rows"),
            P(),
        ),
        check_vma=False,
    )
```

```python
import functools

import jax
import jax.numpy as jnp
from jax import lax
from jax.experimental import pallas as pl
from jax.experimental.pallas import tpu as pltpu
from jax.sharding import PartitionSpec as P

D_MODEL = 2048
MESH = pl.DeviceIdType.MESH
F32, BF16 = jnp.float32, jnp.bfloat16

RAW = 2
FAR = (4, 3, -3, 2, -2, 1, -1, 0)
NEAR = ((1, 0), (1, 1), (-1, 0), (-1, 1))
PEERS = tuple((dz, dc) for dz in FAR for dc in (0, 1) if (dz, dc) != (0, 0))


def exchange(
    gate, up, down, weight, gain,
    out, scale_gate, scale_up, scale_down, router,
    wide, tall, sent, part0, all0, sums, pieces, total, totals, inverse,
    weight_v, gain_v, mine, column, square, plain,
    load, first_s, first_r, sum_s, sum_r, tot_s, tot_r, main_s, main_r, rt_s, rt_r, raw_s, raw_r, both_s, both_r,
):
    owner, me = lax.axis_index("owner"), lax.axis_index("rows")
    z, c = me // 2, lax.rem(me, 2)
    y, x = owner // 4, lax.rem(owner, 4)

    def peer(dz, dc):
        at = lax.rem(z + dz + 8, 8)
        return at * 2 + (1 - c if dc else c)

    loads = []
    for a in range(12):
        source = (gate, up, down)[a // 4].at[a % 4]
        target = wide.at[a] if a < 8 else tall.at[a - 8]
        loads.append(pltpu.make_async_copy(source, target, load.at[a]))
    small = [
        pltpu.make_async_copy(weight, weight_v, load.at[12]),
        pltpu.make_async_copy(gain, gain_v, load.at[13]),
    ]
    loads[0].start()

    barrier = pltpu.get_barrier_semaphore()
    for dz, dc in PEERS:
        pl.semaphore_signal(barrier, inc=1, device_id={"rows": peer(dz, dc)}, device_id_type=MESH)
    xs = [y * 4 + lax.rem(x + k, 4) for k in (2, 1, 3)]
    ys = [lax.rem(y + k, 4) * 4 + x for k in (2, 1, 3)]
    for o in xs + ys:
        pl.semaphore_signal(barrier, inc=1, device_id={"owner": o}, device_id_type=MESH)
    for copy in loads[1:] + small:
        copy.start()

    eye = lax.broadcasted_iota(jnp.int32, (128, 128), 0) == lax.broadcasted_iota(jnp.int32, (128, 128), 1)

    def wide_sum(a):
        return jnp.sum(jnp.abs(wide[a]), axis=0, keepdims=True)

    loads[0].wait()
    row = wide_sum(0)
    for b in range(8):
        part0[b : b + 1, :] = row[:, b * 128 : (b + 1) * 128]
        pieces[b * 2, 0:1, :] = row[:, b * 128 : (b + 1) * 128]
    def add_up():
        for a in range(1, 12):
            loads[a].wait()
            if a < 8:
                row = wide_sum(a)
            for b in range(8):
                if a < 8:
                    piece = row[:, b * 128 : (b + 1) * 128]
                else:
                    column_sum = jnp.sum(jnp.abs(tall[a - 8, b * 128 : (b + 1) * 128, :]), axis=1, keepdims=True)
                    piece = jnp.sum(jnp.where(eye, column_sum, 0.0), axis=0, keepdims=True)
                pieces[b * 2 + a // 6, a % 6 : a % 6 + 1, :] = piece

    pl.when(z < 4)(add_up)
    pl.semaphore_wait(barrier, len(PEERS) + 6)

    def send(source, target, s, r, to):
        pltpu.make_async_remote_copy(
            src_ref=source, dst_ref=target, send_sem=s, recv_sem=r, device_id=to, device_id_type=MESH
        ).start()

    def finish(ref, sem):
        pltpu.make_async_copy(ref, ref, sem).wait()

    for dz, dc in PEERS:
        send(part0, all0.at[me], first_s, first_r, {"rows": peer(dz, dc)})
    all0[me] = part0[...]

    pl.when(z >= 4)(add_up)
    for dz, dc in PEERS:
        to = peer(dz, dc)
        send(pieces.at[to], sums.at[me], sum_s, sum_r, {"rows": to})
    sums[me] = pieces[me]

    for k, (dz, dc) in enumerate(NEAR):
        to = peer(dz, dc)
        rows = pl.ds(pl.multiple_of(to * 64, 64), 64)
        send(tall.at[pl.ds(0, RAW), rows, :], plain.at[k], raw_s, raw_r, {"rows": to})

    for copy in small:
        copy.wait()
    mine[...] = (weight_v[...] * gain_v[...]).astype(BF16)
    column[me] = mine[...]
    for dz, dc in PEERS:
        send(mine, column.at[me], rt_s.at[0], rt_r.at[0], {"rows": peer(dz, dc)})

    finish(all0.at[pl.ds(0, 15)], first_r)
    first = 1.0 / (jnp.sum(all0[...], axis=0) * (1.0 / D_MODEL))
    for b in range(8):
        inverse[0, b] = first[b : b + 1, :]

    def chunk(a, raw=False):
        is_wide = not isinstance(a, tuple)
        a = a if is_wide else a[0]
        pending = None
        for dz in FAR:
            if raw and abs(dz) == 1:
                continue
            at = lax.rem(z + dz + 8, 8)
            rows = pl.ds(pl.multiple_of(at * 128, 128), 128)
            scale = inverse[a, at]
            if is_wide:
                block = (wide[a, :, rows] * scale).astype(BF16).T
            else:
                per_row = jnp.sum(jnp.where(eye, scale, 0.0), axis=1, keepdims=True)
                block = (tall[a - 8, rows, :] * per_row).astype(BF16)
            sent[a, rows, :] = block
            if pending is not None:
                launch(a, pending)
            pending = dz
        launch(a, pending)
        own = sent[a, pl.ds(pl.multiple_of(me * 64, 64), 64), :]
        out[a, :, pl.ds(pl.multiple_of(me * 128, 128), 128)] = own

    def launch(a, dz):
        group = a // 4 + (a >= 8 + RAW)
        for dc in (0, 1):
            if (dz, dc) == (0, 0):
                continue
            to = peer(dz, dc)
            send(
                sent.at[a, pl.ds(pl.multiple_of(to * 64, 64), 64), :],
                out.at[a, :, pl.ds(pl.multiple_of(me * 128, 128), 128)],
                main_s.at[group], main_r.at[group], {"rows": to},
            )

    def reduce_sums():
        finish(sums.at[pl.ds(0, 15)], sum_r)
        total[...] = jnp.sum(sums[...], axis=0)
        totals[c, z] = total[...]
        for dz in FAR[:-1]:
            send(total, totals.at[c, z], tot_s, tot_r, {"rows": peer(dz, 0)})

    reduce_sums()
    chunk(0)

    finish(column.at[pl.ds(0, 15)], rt_r.at[0])
    for r in range(16):
        square[y, x, :, r * 128 : (r + 1) * 128] = column[r]

    finish(totals.at[0, pl.ds(0, 7)], tot_r)
    send(totals.at[c], totals.at[c], both_s, both_r, {"rows": peer(0, 1)})
    finish(totals.at[0], both_r)
    for a in range(12):
        for b in range(8):
            if a:
                inverse[a, b] = 1.0 / (totals[a // 6, b, a % 6 : a % 6 + 1, :] * (1.0 / D_MODEL))

    for o in xs:
        send(square.at[y, x], square.at[y, x], rt_s.at[1], rt_r.at[1], {"owner": o})

    @pl.loop(1, 8)
    def _(a):
        chunk(a)

    finish(square.at[0, pl.ds(0, 3)], rt_r.at[1])
    finish(square.at[0, pl.ds(0, 3)], rt_s.at[1])
    for o in ys:
        send(square.at[y], square.at[y], rt_s.at[2], rt_r.at[2], {"owner": o})

    @pl.loop(8, 8 + RAW)
    def _(a):
        chunk((a,), raw=True)

    @pl.loop(8 + RAW, 12)
    def _(a):
        chunk((a,))

    halves = []
    for h in range(2):
        v = totals[h, z] * (1.0 / D_MODEL)
        halves.append(jnp.where(c == 1, pltpu.roll(v, 64, 1), v)[:, :64])
    scale_gate[...] = halves[0][:4]
    scale_up[...] = jnp.concatenate([halves[0][4:], halves[1][:2]], axis=0)
    scale_down[...] = halves[1][2:]

    finish(plain, raw_r)
    for e in range(RAW):
        last = 1.0 / halves[1][2 + e : 3 + e]
        last = jnp.concatenate([last, last], axis=1)
        per_row = jnp.sum(jnp.where(eye, last, 0.0), axis=1, keepdims=True)[:64]
        for k, (dz, dc) in enumerate(NEAR):
            lanes = pl.ds(pl.multiple_of(peer(-dz, dc) * 128, 128), 128)
            out[8 + e, :, lanes] = (plain[k, e] * per_row).astype(BF16)

    finish(square.at[pl.ds(0, 3)], rt_r.at[2])
    for j in range(4):
        rows16 = jnp.concatenate([square[j, i].astype(F32) for i in range(4)], axis=0)
        router[j * 16 : (j + 1) * 16, :] = rows16.astype(BF16)

    finish(all0.at[pl.ds(0, 15)], first_s)
    finish(sums.at[pl.ds(0, 15)], sum_s)
    finish(totals.at[0, pl.ds(0, 7)], tot_s)
    finish(totals.at[0], both_s)
    finish(column.at[pl.ds(0, 15)], rt_s.at[0])
    finish(square.at[pl.ds(0, 3)], rt_s.at[2])
    finish(plain, raw_s)
    everything = [
        out.at[pl.ds(0, 4), :, pl.ds(0, 1920)], out.at[pl.ds(4, 4), :, pl.ds(0, 1920)],
        out.at[pl.ds(8, RAW), :, pl.ds(0, 1408)], out.at[pl.ds(8 + RAW, 4 - RAW), :, pl.ds(0, 1920)],
    ]
    for i, ref in enumerate(everything):
        finish(ref, main_s.at[i])
        finish(ref, main_r.at[i])


def place(out, scale_gate, scale_up, scale_down, router, *rest):
    outs, sem = rest[:7], rest[7]
    sources = [out.at[pl.ds(0, 4)], out.at[pl.ds(4, 4)], out.at[pl.ds(8, 4)], scale_gate, scale_up, scale_down, router]
    copies = [pltpu.make_async_copy(s, d, sem.at[i]) for i, (s, d) in enumerate(zip(sources, outs))]
    for copy in copies:
        copy.start()
    for copy in copies:
        copy.wait()


def local(train_gate, train_up, train_down, router_weight, router_gain):
    anywhere = pl.BlockSpec(memory_space=pl.ANY)
    vmem = pl.BlockSpec(memory_space=pltpu.VMEM)
    shapes = [((12, 64, 2048), BF16), ((4, 64), F32), ((4, 64), F32), ((4, 64), F32), ((64, 2048), BF16)]
    dma = pltpu.SemaphoreType.DMA
    kept = pl.pallas_call(
        exchange,
        out_shape=[pltpu.VMEM(s, d) for s, d in shapes],
        in_specs=[pl.BlockSpec(memory_space=pltpu.HBM)] * 5,
        out_specs=[vmem] * 5,
        scratch_shapes=[
            pltpu.VMEM((8, 128, 1024), F32),
            pltpu.VMEM((4, 1024, 128), F32),
            pltpu.VMEM((12, 1024, 128), BF16),
            pltpu.VMEM((8, 128), F32),
            pltpu.VMEM((16, 8, 128), F32),
            pltpu.VMEM((16, 6, 128), F32),
            pltpu.VMEM((16, 6, 128), F32),
            pltpu.VMEM((6, 128), F32),
            pltpu.VMEM((2, 8, 6, 128), F32),
            pltpu.VMEM((12, 8, 1, 128), F32),
            pltpu.VMEM((4, 128), F32),
            pltpu.VMEM((1, 128), F32),
            pltpu.VMEM((4, 128), BF16),
            pltpu.VMEM((16, 4, 128), BF16),
            pltpu.VMEM((4, 4, 4, 2048), BF16),
            pltpu.VMEM((4, RAW, 64, 128), F32),
            dma((14,)), dma, dma, dma, dma, dma, dma, dma((4,)), dma((4,)), dma((3,)), dma((3,)), dma, dma, dma, dma,
        ],
        compiler_params=pltpu.CompilerParams(
            collective_id=0, has_side_effects=True, vmem_limit_bytes=58 << 20
        ),
    )(train_gate, train_up, train_down, router_weight.T, router_gain[None])
    outs = [((4, 64, 2048), BF16)] * 3 + [((4, 64), F32)] * 3 + [((64, 2048), BF16)]
    gate, up, down, scale_gate, scale_up, scale_down, router = pl.pallas_call(
        place,
        out_shape=[jax.ShapeDtypeStruct(s, d) for s, d in outs],
        in_specs=[vmem] * 5,
        out_specs=[pl.BlockSpec(memory_space=pltpu.HBM)] * 7,
        scratch_shapes=[dma((7,))],
        compiler_params=pltpu.CompilerParams(vmem_limit_bytes=4 << 20),
    )(*[pltpu.with_memory_space_constraint(k, pltpu.VMEM) for k in kept])
    return (
        jnp.swapaxes(gate, 1, 2), jnp.swapaxes(up, 1, 2), down, scale_gate, scale_up, scale_down, router.T,
    )


def solution(mesh):
    return jax.shard_map(
        local,
        mesh=mesh,
        in_specs=(
            P("owner", "rows", None),
            P("owner", "rows", None),
            P("owner", None, "rows"),
            P("rows", "owner"),
            P("rows"),
        ),
        out_specs=(
            P("owner", None, "rows"),
            P("owner", None, "rows"),
            P("owner", "rows", None),
            P("owner", "rows"),
            P("owner", "rows"),
            P("owner", "rows"),
            P(),
        ),
        check_vma=False,
    )
```
